32 devices in a mesh: coil: 8 (over y, x, core), kz: 4 (over z).
Axes of the slice: x: 2, y: 2, z: 4, core: 2. Of those that a mesh axis runs over, the one named last changes fastest.
Arguments:
- kdata: bfloat16 [2, 64, 8, 256, 512], P(None, 'kz', 'coil'), may hold values from -6 to 6
- spoke_angle: int32 [256], replicated, may hold values from 0 to 63
- spoke_count: int32 [64], P('kz'), may hold values from 128 to 256
- block_index: int32 [64, 4], replicated, may hold values from 0 to 511
- interp: bfloat16 [64, 4, 128, 128], replicated, may hold values from -0.5 to 0.5
- sens_maps: bfloat16 [2, 8, 256, 256], P(None, 'coil'), may hold values from -5 to 5
Outputs:
- image: float32 [2, 64, 256, 256], P(None, 'kz', 'coil')
The draws below stay inside these ranges and needn't reach their ends.
Inputs may be any that keep to these rules, and one draw needn't show every extreme that they name: Partition p uses its first spoke_count[p] spokes. `block_index`: several segments may hit the same grid block.
All inputs are finite; a program needn't handle non-finite values.
Results may differ from the reference program's by a relative error of at most 0.0059.
Values sent between devices are 32-bit elements; how exact they have to be, the bound alone decides.
A program may use at most 128 MiB of HBM per device.

```python
import jax
import jax.numpy as jnp
from jax import lax

N = 256
SAMPLES = 512
SEG_LEN = 128
SEGS = 4
BLOCKS = 512
SPOKES = 256
ANGLES = 64
KZ = 64
COILS = 8


def place_ends(values, key, smallest, largest):
    spot = [jax.random.randint(jax.random.fold_in(key, axis), (), 0, length) for axis, length in enumerate(values.shape)]
    main_axis = values.shape.index(max(values.shape))
    next_to = spot[:main_axis] + [(spot[main_axis] + 1) % values.shape[main_axis]] + spot[main_axis + 1:]
    return values.at[tuple(spot)].set(smallest).at[tuple(next_to)].set(largest)


def level_of(stream_key, dims, cuts, smallest, largest):
    def one(dim, blocks):
        steps = jax.random.uniform(jax.random.fold_in(jax.random.fold_in(stream_key, 6), dim), (blocks,), jnp.float32, smallest / len(cuts), largest / len(cuts))
        return jnp.repeat(jnp.exp(steps), dims[dim] // blocks).reshape((-1,) + (1,) * (len(dims) - dim - 1))

    factor_of = one(*cuts[0])
    for cut in cuts[1:]:
        factor_of = factor_of * one(*cut)
    return factor_of


def centred(rng, shape, width, limit, cuts=(), kind=jnp.bfloat16):
    values = width * jax.random.normal(rng, shape, jnp.float32)
    if cuts:
        values = values * level_of(rng, shape, cuts, -0.22, 0.18)
    return jnp.clip(values, -limit, limit).astype(kind)


def setup_inputs(seed: int = 0) -> dict:
    arg_keys = jax.random.split(jax.random.key(seed), 7)
    return {
        "kdata": centred(arg_keys[0], (2, KZ, COILS, SPOKES, SAMPLES), 1.0, 6.0, ((1, 4), (2, 8))),
        "spoke_angle": place_ends(jax.random.randint(arg_keys[1], (SPOKES,), 0, ANGLES), jax.random.fold_in(arg_keys[1], 1), 0, ANGLES - 1).astype(jnp.int32),
        "spoke_count": place_ends(jax.random.randint(arg_keys[2], (KZ,), SPOKES // 2, SPOKES + 1), jax.random.fold_in(arg_keys[2], 1), SPOKES // 2, SPOKES).astype(jnp.int32),
        "block_index": place_ends(jax.random.randint(arg_keys[3], (ANGLES, SEGS), 0, BLOCKS), jax.random.fold_in(arg_keys[3], 1), 0, BLOCKS - 1).astype(jnp.int32),
        "interp": centred(arg_keys[4], (ANGLES, SEGS, SEG_LEN, SEG_LEN), SEG_LEN ** -0.5, 0.5),
        "sens_maps": centred(arg_keys[5], (2, COILS, N, N), (COILS ** -0.5), 5.0, ((1, 8),)),
    }


def dft_tables(length, dtype):
    index = jnp.arange(length, dtype=jnp.int32)
    product = index[:, None] * index[None, :] % length
    phase = product.astype(jnp.float32) * (2.0 * jnp.pi / length)
    scale = 1.0 / jnp.sqrt(jnp.float32(length))
    return ((jnp.cos(phase) * scale).astype(dtype), (jnp.sin(phase) * scale).astype(dtype))

def spoke_weights(spoke_count, spoke_angle, angles, spokes):
    position = jnp.arange(spokes, dtype=jnp.int32)
    used = position[None, :] < spoke_count[:, None]
    match = spoke_angle[:, None] == jnp.arange(angles, dtype=jnp.int32)[None, :]
    return (used[:, :, None] & match[None, :, :]).astype(jnp.bfloat16)

def coil_image(data, weights, interp, block_index, cos_t, sin_t):
    f32 = jnp.float32
    binned = jnp.einsum('rpsn,psa->rpan', data.astype(f32), weights.astype(f32)).astype(jnp.bfloat16)
    rdim, pdim, adim, mdim = binned.shape
    seg = interp.shape[2]
    gdim = mdim // seg
    side = cos_t.shape[0]
    pieces = binned.reshape(rdim, pdim, adim, gdim, seg)
    contrib = jnp.einsum('rpagj,agjt->rpagt', pieces.astype(f32), interp.astype(f32))
    flat = jnp.zeros((rdim, pdim, side * side // seg, seg), f32)
    flat = flat.at[:, :, block_index.reshape(-1)].add(contrib.reshape(rdim, pdim, adim * gdim, seg))
    grid = flat.reshape(rdim, pdim, side, side).astype(jnp.bfloat16)
    cosf = cos_t.astype(f32)
    sinf = sin_t.astype(f32)
    grid_re = grid[0].astype(f32)
    grid_im = grid[1].astype(f32)
    half_re = jnp.einsum('ky,pyx->pkx', cosf, grid_re) + jnp.einsum('ky,pyx->pkx', sinf, grid_im)
    half_im = jnp.einsum('ky,pyx->pkx', cosf, grid_im) - jnp.einsum('ky,pyx->pkx', sinf, grid_re)
    half_re = half_re.astype(jnp.bfloat16).astype(f32)
    half_im = half_im.astype(jnp.bfloat16).astype(f32)
    out_re = jnp.einsum('pkx,mx->pkm', half_re, cosf) + jnp.einsum('pkx,mx->pkm', half_im, sinf)
    out_im = jnp.einsum('pkx,mx->pkm', half_im, cosf) - jnp.einsum('pkx,mx->pkm', half_re, sinf)
    return jnp.stack([out_re, out_im])

def conj_product(sens, image):
    real_part = sens[0] * image[0] + sens[1] * image[1]
    imag_part = sens[0] * image[1] - sens[1] * image[0]
    return jnp.stack([real_part, imag_part])

def reference(kdata, spoke_angle, spoke_count, block_index, interp, sens_maps):
    cos_t, sin_t = dft_tables(N, jnp.bfloat16)
    weights = spoke_weights(spoke_count, spoke_angle, ANGLES, SPOKES)

    def per_coil(total, coil_id):
        data = lax.dynamic_index_in_dim(kdata, coil_id, 2, keepdims=False)
        image_c = coil_image(data, weights, interp, block_index, cos_t, sin_t)
        sens = lax.dynamic_index_in_dim(sens_maps, coil_id, 1, keepdims=False).astype(jnp.float32)
        return (total + conj_product(sens[:, None], image_c), None)
    start = jnp.zeros((2, KZ, N, N), jnp.float32)
    combined, unused = lax.scan(per_coil, start, jnp.arange(COILS, dtype=jnp.int32))
    cos_z, sin_z = dft_tables(KZ, jnp.float32)
    high = lax.Precision.HIGHEST
    image_re = jnp.einsum('zk,kyx->zyx', cos_z, combined[0], precision=high) + jnp.einsum('zk,kyx->zyx', sin_z, combined[1], precision=high)
    image_im = jnp.einsum('zk,kyx->zyx', cos_z, combined[1], precision=high) - jnp.einsum('zk,kyx->zyx', sin_z, combined[0], precision=high)
    return jnp.stack([image_re, image_im])
```

```python
import functools
import math

import jax
import jax.numpy as jnp
from jax import lax
from jax.experimental import pallas as pl
from jax.experimental.pallas import tpu as pltpu
from jax.sharding import PartitionSpec as P

F32 = jnp.float32
BF16 = jnp.bfloat16
SUB = 2


def cos_sin(product, length, dtype):
    phase = (product % length).astype(F32) * (2.0 * jnp.pi / length)
    scale = 1.0 / jnp.sqrt(F32(length))
    return ((jnp.cos(phase) * scale).astype(dtype), (jnp.sin(phase) * scale).astype(dtype))


def halving_orders(bits):
    first = list(range(bits))
    return [first, first[:1] + first[:0:-1]]


def kernel(bits, groups, parts, rows, side, *refs):
    contrib, ymat, xmat, sens, twiddle, out = refs[:6]
    weighted, gathered = refs[6:8]
    inbox = refs[8 : 8 + bits]
    half_send, half_recv, ring_send, ring_recv = refs[8 + bits :]
    blocks = 1 << bits
    orders = halving_orders(bits)
    steps = parts // SUB
    coil = lax.axis_index("coil")
    kz = lax.axis_index("kz")
    my_bit = [(coil // (1 << bit)) % 2 for bit in range(bits)]
    partner = [coil + (1 - 2 * my_bit[bit]) * (1 << bit) for bit in range(bits)]
    right = (kz + 1) % groups
    left = (kz + groups - 1) % groups

    barrier = pltpu.get_barrier_semaphore()
    for bit in range(bits):
        pl.semaphore_signal(barrier, 1, device_id={"coil": partner[bit]})
    pl.semaphore_signal(barrier, 1, device_id={"kz": right})
    pl.semaphore_signal(barrier, 1, device_id={"kz": left})
    pl.semaphore_wait(barrier, bits + 2)

    def kept_start(order, stage):
        start = 0
        for s in range(stage):
            start = start + my_bit[order[s]] * (blocks >> (s + 1))
        return start

    def half_copy(part, sub, stage):
        order = orders[sub % 2]
        bit = order[stage]
        size = blocks >> (stage + 1)
        start = kept_start(order, stage) + (1 - my_bit[bit]) * size
        return pltpu.make_async_remote_copy(
            src_ref=weighted.at[part, pl.ds(start, size)],
            dst_ref=inbox[stage].at[part],
            send_sem=half_send.at[stage, part],
            recv_sem=half_recv.at[stage, part],
            device_id={"coil": partner[bit]},
        )

    def add_inbox(part, sub, stage):
        size = blocks >> (stage + 1)
        start = kept_start(orders[sub % 2], stage + 1)
        total = weighted[part, pl.ds(start, size)] + inbox[stage][part]
        if stage < bits - 1:
            weighted[part, pl.ds(start, size)] = total
        else:
            gathered[part, 0] = total[0]

    far = groups // 2

    def ring_copies(part, hop):
        copies = []
        for way in range(2):
            if way == 0:
                source, target, to = hop - 1, hop, right
            else:
                source, target, to = (groups - hop + 1) % groups, groups - hop, left
            if hop == far:
                src, dst = gathered.at[part, source, way], gathered.at[part, target, way]
            else:
                src, dst = gathered.at[part, source], gathered.at[part, target]
            copies.append(
                pltpu.make_async_remote_copy(
                    src_ref=src,
                    dst_ref=dst,
                    send_sem=ring_send.at[hop - 1, way, part],
                    recv_sem=ring_recv.at[hop - 1, way, part],
                    device_id={"kz": to},
                )
            )
        return copies

    def compute(step):
        first = step * SUB
        data = jnp.concatenate([contrib[first + s] for s in range(SUB)], axis=1)
        seg = data.shape[1] // SUB
        halves = [
            jnp.dot(ymat[h], data, preferred_element_type=F32).astype(BF16)
            for h in range(side // seg)
        ]
        s_re = sens[0].astype(F32)
        s_im = sens[1].astype(F32)
        for s in range(SUB):
            pieces = [h[r * side : (r + 1) * side, s * seg : (s + 1) * seg] for r in range(2) for h in halves]
            image = jnp.dot(jnp.concatenate(pieces, axis=1), xmat[...], preferred_element_type=F32)
            i_re, i_im = image[:, :side], image[:, side:]
            result = [s_re * i_re + s_im * i_im, s_re * i_im - s_im * i_re]
            order = orders[s % 2]
            for block in range(blocks):
                place = 0
                for bit in order:
                    place = place * 2 + (block >> bit) % 2
                for r in range(2):
                    weighted[first + s, place, r] = result[r][block * rows : (block + 1) * rows]

    def transform(step):
        group = 8
        for row in range(0, rows, group):
            inner = []
            for s in range(SUB):
                x = [[gathered[step * SUB + s, j, r, row : row + group] for r in range(2)] for j in range(groups)]
                per_q = []
                for q in range(groups):
                    re = im = None
                    for j in range(groups):
                        angle = 2.0 * math.pi * (q * j % groups) / groups
                        c, d = round(math.cos(angle), 12), round(math.sin(angle), 12)
                        for coef, a, b in ((c, x[j][0], x[j][1]), (d, -x[j][1], x[j][0])):
                            if coef == 0.0:
                                continue
                            ta = a if coef == 1.0 else a * F32(coef)
                            tb = b if coef == 1.0 else b * F32(coef)
                            re = ta if re is None else re + ta
                            im = tb if im is None else im + tb
                    per_q.append((re, im))
                inner.append(per_q)
            for z in range(parts):
                a_re = out[0, z, row : row + group]
                a_im = out[1, z, row : row + group]
                for s in range(SUB):
                    k = step * SUB + s
                    c, d = twiddle[0, k, z], twiddle[1, k, z]
                    re, im = inner[s][z % groups]
                    a_re = a_re + (c * re + d * im)
                    a_im = a_im + (c * im - d * re)
                out[0, z, row : row + group] = a_re
                out[1, z, row : row + group] = a_im

    out[...] = jnp.zeros_like(out)
    lags = [0, 1]
    for _ in range(bits + far - 1):
        lags.append(lags[-1] + 2)

    def tick(t, carry):
        def at(index, body):
            step = t - lags[index]

            @pl.when((step >= 0) & (step < steps))
            def _():
                body(step)

        def begin(step):
            compute(step)
            for s in range(SUB):
                half_copy(step * SUB + s, s, 0).start()

        at(0, begin)
        for stage in range(bits):

            def reduce_stage(step, stage=stage):
                for s in range(SUB):
                    part = step * SUB + s
                    half_copy(part, s, stage).wait_recv()
                    add_inbox(part, s, stage)
                    if stage < bits - 1:
                        half_copy(part, s, stage + 1).start()
                    else:
                        for copy in ring_copies(part, 1):
                            copy.start()

            at(1 + stage, reduce_stage)
        for hop in range(1, far + 1):

            def ring_stage(step, hop=hop):
                for s in range(SUB):
                    part = step * SUB + s
                    for copy in ring_copies(part, hop):
                        copy.wait_recv()
                    if hop < far:
                        for copy in ring_copies(part, hop + 1):
                            copy.start()
                if hop == far:
                    transform(step)

            at(bits + hop, ring_stage)
        return carry

    lax.fori_loop(0, steps + lags[-1], tick, 0)

    def finish(step, carry):
        for s in range(SUB):
            part = step * SUB + s
            for stage in range(bits):
                half_copy(part, s, stage).wait_send()
            for hop in range(1, far + 1):
                for copy in ring_copies(part, hop):
                    copy.wait_send()
        return carry

    lax.fori_loop(0, steps, finish, 0)


def per_device(kdata, spoke_angle, spoke_count, block_index, interp, sens_maps):
    side = sens_maps.shape[2]
    parts = kdata.shape[1]
    spokes = kdata.shape[3]
    angles, segs, seg = interp.shape[:3]
    coils = lax.axis_size("coil")
    groups = lax.axis_size("kz")
    bits = coils.bit_length() - 1
    rows = side // coils
    length = parts * groups
    kz = lax.axis_index("kz")

    position = jnp.arange(spokes, dtype=jnp.int32)
    used = position[None, :] < spoke_count[:, None]
    match = spoke_angle[:, None] == jnp.arange(angles, dtype=jnp.int32)[None, :]
    weights = (used[:, :, None] & match[None, :, :]).astype(BF16)
    binned = jnp.einsum("rpsn,psa->rpan", kdata[:, :, 0], weights, preferred_element_type=F32).astype(BF16)
    pieces = binned.reshape(2, parts, angles, segs, seg)
    contrib = jnp.einsum("rpagj,agjt->pragt", pieces, interp, preferred_element_type=F32).astype(BF16)
    hits = angles * segs
    contrib = contrib.reshape(parts, 2 * hits, seg)

    across = side // seg
    index = jnp.arange(side, dtype=jnp.int32)
    where = block_index.reshape(-1)
    hit_y = where // across
    hit_x = where % across
    cos_y, sin_y = cos_sin(index[:, None] * hit_y[None, :], side, F32)
    here = (jnp.arange(across, dtype=jnp.int32)[:, None, None] == hit_x).astype(F32)
    cos_y, sin_y = cos_y * here, sin_y * here
    ymat = jnp.concatenate(
        [jnp.concatenate([cos_y, sin_y], 2), jnp.concatenate([-sin_y, cos_y], 2)], 1
    ).astype(BF16)
    cos_x, sin_x = cos_sin(index[:, None] * index[None, :], side, F32)
    xmat = jnp.concatenate(
        [jnp.concatenate([cos_x, -sin_x], 1), jnp.concatenate([sin_x, cos_x], 1)], 0
    ).astype(BF16)
    mine = kz * parts + jnp.arange(parts, dtype=jnp.int32)
    twiddle = jnp.stack(cos_sin(mine[:, None] * mine[None, :], length, F32))

    block = (2, rows, side)
    vmem = pl.BlockSpec(memory_space=pltpu.VMEM)
    far = groups // 2
    scratch = [
        pltpu.VMEM((parts, coils) + block, F32),
        pltpu.VMEM((parts, groups) + block, F32),
    ]
    scratch += [pltpu.VMEM((parts, coils >> (s + 1)) + block, F32) for s in range(bits)]
    scratch += [pltpu.SemaphoreType.DMA((bits, parts))] * 2
    scratch += [pltpu.SemaphoreType.DMA((far, 2, parts))] * 2
    return pl.pallas_call(
        functools.partial(kernel, bits, groups, parts, rows, side),
        out_shape=jax.ShapeDtypeStruct((2, parts, rows, side), F32),
        in_specs=[vmem] * 4 + [pl.BlockSpec(memory_space=pltpu.SMEM)],
        out_specs=vmem,
        scratch_shapes=scratch,
        compiler_params=pltpu.CompilerParams(
            collective_id=0, has_side_effects=True, vmem_limit_bytes=60 * 1024 * 1024
        ),
        name="combine",
    )(contrib, ymat, xmat, sens_maps[:, 0], twiddle)


def solution(mesh):
    placed = (
        P(None, "kz", "coil", None, None),
        P(),
        P("kz"),
        P(),
        P(),
        P(None, "coil", None, None),
    )
    return jax.shard_map(
        per_device,
        mesh=mesh,
        in_specs=placed,
        out_specs=P(None, "kz", "coil", None),
        check_vma=False,
    )
```

```python
import functools
import math

import jax
import jax.numpy as jnp
from jax import lax
from jax.experimental import pallas as pl
from jax.experimental.pallas import tpu as pltpu
from jax.sharding import PartitionSpec as P

F32 = jnp.float32
BF16 = jnp.bfloat16
SUB = 2
SUBLANE, LANE = 8, 128


def cos_sin(product, length, dtype):
    phase = (product % length).astype(F32) * (2.0 * jnp.pi / length)
    scale = 1.0 / jnp.sqrt(F32(length))
    return ((jnp.cos(phase) * scale).astype(dtype), (jnp.sin(phase) * scale).astype(dtype))


def halving_orders(bits):
    first = list(range(bits))
    return [first, first[:1] + first[:0:-1]]


def kernel(bits, groups, parts, rows, side, *refs):
    contrib, ymat, xmat, sens, twiddle, out = refs[:6]
    weighted, raw, part_out, part_in = refs[6:10]
    inbox = refs[10 : 10 + bits]
    first_send, first_recv, half_send, half_recv, line_send, line_recv = refs[10 + bits :]
    blocks = 1 << bits
    orders = halving_orders(bits)
    lanes = side // LANE
    steps = rows // SUBLANE
    coil = lax.axis_index("coil")
    kz = lax.axis_index("kz")
    my_bit = [(coil // (1 << bit)) % 2 for bit in range(bits)]
    partner = [coil + (1 - 2 * my_bit[bit]) * (1 << bit) for bit in range(bits)]
    last = groups - 1
    inner = (kz > 0) & (kz < last)
    outer = (kz == 0) | (kz == last)
    inward = jnp.where(kz < 2, kz + 1, kz - 1)
    outward = jnp.where(kz < 2, 0, last)
    far_end = last - outward

    barrier = pltpu.get_barrier_semaphore()
    for bit in range(bits):
        pl.semaphore_signal(barrier, 1, device_id={"coil": partner[bit]})
    pl.semaphore_signal(barrier, 1, device_id={"kz": (kz + 1) % groups})
    pl.semaphore_signal(barrier, 1, device_id={"kz": (kz + groups - 1) % groups})
    pl.semaphore_wait(barrier, bits + 2)

    def kept_start(order, stage):
        start = 0
        for s in range(stage):
            start = start + my_bit[order[s]] * (blocks >> (s + 1))
        return start

    half = blocks // 2

    def first_copy(pair):
        span = pl.ds(pair * SUB, SUB)
        return pltpu.make_async_remote_copy(
            src_ref=weighted.at[:, pl.ds((1 - my_bit[0]) * half, half), span],
            dst_ref=inbox[0].at[:, :, span],
            send_sem=first_send.at[pair],
            recv_sem=first_recv.at[pair],
            device_id={"coil": partner[0]},
        )

    def half_copy(chunk, lane, stage):
        order = orders[lane % 2]
        bit = order[stage]
        size = blocks >> (stage + 1)
        start = kept_start(order, stage) + (1 - my_bit[bit]) * size
        return pltpu.make_async_remote_copy(
            src_ref=weighted.at[chunk, pl.ds(start, size)],
            dst_ref=inbox[stage].at[chunk],
            send_sem=half_send.at[stage - 1, chunk],
            recv_sem=half_recv.at[stage - 1, chunk],
            device_id={"coil": partner[bit]},
        )

    def add_inbox(chunk, lane, stage):
        size = blocks >> (stage + 1)
        start = kept_start(orders[lane % 2], stage + 1)
        for b in range(size):
            total = weighted[chunk, start + b] + inbox[stage][chunk, b]
            if stage < bits - 1:
                weighted[chunk, start + b] = total
            else:
                raw[chunk, kz] = total

    def line_copy(kind, chunk, src, dst, to):
        return pltpu.make_async_remote_copy(
            src_ref=src,
            dst_ref=dst,
            send_sem=line_send.at[kind, chunk],
            recv_sem=line_recv.at[kind, chunk],
            device_id={"kz": to},
        )

    def from_outer(chunk, source):
        return line_copy(0, chunk, raw.at[chunk, source], raw.at[chunk, source], inward)

    def from_inner(chunk, source):
        return line_copy(1, chunk, raw.at[chunk, source], raw.at[chunk, source], inward)

    def forward(chunk, source):
        return line_copy(2, chunk, raw.at[chunk, source], raw.at[chunk, source], inward)

    def partial(chunk):
        return line_copy(3, chunk, part_out.at[chunk], part_in.at[chunk], outward)

    def compute(pair):
        first = pair * SUB
        data = jnp.concatenate([contrib[first + s] for s in range(SUB)], axis=1)
        seg = data.shape[1] // SUB
        halves = [
            jnp.dot(ymat[h], data, preferred_element_type=F32).astype(BF16)
            for h in range(side // seg)
        ]
        s_re = sens[0].astype(F32)
        s_im = sens[1].astype(F32)
        for s in range(SUB):
            pieces = [h[r * side : (r + 1) * side, s * seg : (s + 1) * seg] for r in range(2) for h in halves]
            image = jnp.dot(jnp.concatenate(pieces, axis=1), xmat[...], preferred_element_type=F32)
            i_re, i_im = image[:, :side], image[:, side:]
            result = [s_re * i_re + s_im * i_im, s_re * i_im - s_im * i_re]
            for block in range(blocks):
                for lane in range(lanes):
                    place = 0
                    for bit in orders[lane % 2]:
                        place = place * 2 + (block >> bit) % 2
                    for step in range(steps):
                        top = block * rows + step * SUBLANE
                        for r in range(2):
                            weighted[step * lanes + lane, place, first + s, r] = result[r][
                                top : top + SUBLANE, lane * LANE : (lane + 1) * LANE
                            ]

    def transform(chunk, sources, table, store):
        for q in range(groups):
            sums = []
            for k in range(parts):
                re = im = None
                for j in sources:
                    angle = 2.0 * math.pi * (q * j % groups) / groups
                    c, d = round(math.cos(angle), 12), round(math.sin(angle), 12)
                    x_re, x_im = raw[chunk, j, k, 0], raw[chunk, j, k, 1]
                    for coef, a, b in ((c, x_re, x_im), (d, x_im, -x_re)):
                        if coef == 0.0:
                            continue
                        ta = a if coef == 1.0 else a * F32(coef)
                        tb = b if coef == 1.0 else b * F32(coef)
                        re = ta if re is None else re + ta
                        im = tb if im is None else im + tb
                sums.append((re, im))
            for z in range(q, parts, groups):
                a_re = a_im = None
                for k in range(parts):
                    c, d = twiddle[2 * table, k, z], twiddle[2 * table + 1, k, z]
                    re, im = sums[k]
                    t_re, t_im = c * re + d * im, c * im - d * re
                    a_re = t_re if a_re is None else a_re + t_re
                    a_im = t_im if a_im is None else a_im + t_im
                store(z, a_re, a_im)

    def spot(step, lane):
        return pl.ds(pl.multiple_of(step * SUBLANE, SUBLANE), SUBLANE), pl.ds(lane * LANE, LANE)

    def into_out(step, lane):
        y, x = spot(step, lane)

        def store(z, re, im):
            out[0, z, y, x] = re
            out[1, z, y, x] = im

        return store

    def into_partial(chunk):
        def store(z, re, im):
            part_out[chunk, z, 0] = re
            part_out[chunk, z, 1] = im

        return store

    def each_pair(pair, carry):
        compute(pair)
        first_copy(pair).start()
        return carry

    pairs = parts // SUB
    lax.fori_loop(0, pairs, each_pair, 0)

    def first_wait(pair, carry):
        first_copy(pair).wait_recv()
        return carry

    lax.fori_loop(0, pairs, first_wait, 0)

    def reduce_stage(stage, step):
        for lane in range(lanes):
            chunk = step * lanes + lane
            if stage:
                half_copy(chunk, lane, stage).wait_recv()
            add_inbox(chunk, lane, stage)
            if stage < bits - 1:
                half_copy(chunk, lane, stage + 1).start()
            else:

                @pl.when(outer)
                def _():
                    from_outer(chunk, kz).start()

                @pl.when(inner)
                def _():
                    from_inner(chunk, kz).start()

    def relay_stage(step):
        for lane in range(lanes):
            chunk = step * lanes + lane

            @pl.when(inner)
            def _():
                from_outer(chunk, outward).wait_recv()
                forward(chunk, outward).start()

            for end in (0, last):

                @pl.when(kz == end)
                def _(end=end):
                    transform(chunk, [end], 0, into_out(step, lane))

    def combine_stage(step):
        for lane in range(lanes):
            chunk = step * lanes + lane

            @pl.when(inner)
            def _():
                from_inner(chunk, inward).wait_recv()
                forward(chunk, far_end).wait_recv()

            for place, end in ((1, 0), (last - 1, last)):

                @pl.when(kz == place)
                def _(end=end):
                    transform(chunk, [j for j in range(groups) if j != end], 1, into_partial(chunk))
                    partial(chunk).start()

            @pl.when(inner)
            def _():
                transform(chunk, list(range(groups)), 0, into_out(step, lane))

    def finish_stage(step):
        for lane in range(lanes):
            chunk = step * lanes + lane

            @pl.when(outer)
            def _():
                partial(chunk).wait_recv()
                y, x = spot(step, lane)
                for r in range(2):
                    out[r, :, y, x] = out[r, :, y, x] + part_in[chunk, :, r]

    def tick(t, carry):
        def at(lag, body):
            step = t - lag

            @pl.when((step >= 0) & (step < steps))
            def _():
                body(step)

        at(bits, relay_stage)
        for stage in range(bits - 1, -1, -1):
            at(stage, functools.partial(reduce_stage, stage))
        at(bits + 1, combine_stage)
        at(bits + 2, finish_stage)
        return carry

    lax.fori_loop(0, steps + bits + 2, tick, 0)

    def drain_first(pair, carry):
        first_copy(pair).wait_send()
        return carry

    lax.fori_loop(0, pairs, drain_first, 0)

    def drain(step, carry):
        for lane in range(lanes):
            chunk = step * lanes + lane
            for stage in range(1, bits):
                half_copy(chunk, lane, stage).wait_send()

            @pl.when(outer)
            def _():
                from_outer(chunk, kz).wait_send()

            @pl.when(inner)
            def _():
                from_inner(chunk, kz).wait_send()
                forward(chunk, outward).wait_send()
                partial(chunk).wait_send()

        return carry

    lax.fori_loop(0, steps, drain, 0)


def per_device(kdata, spoke_angle, spoke_count, block_index, interp, sens_maps):
    side = sens_maps.shape[2]
    parts = kdata.shape[1]
    spokes = kdata.shape[3]
    angles, segs, seg = interp.shape[:3]
    coils = lax.axis_size("coil")
    groups = lax.axis_size("kz")
    bits = coils.bit_length() - 1
    rows = side // coils
    length = parts * groups
    kz = lax.axis_index("kz")

    position = jnp.arange(spokes, dtype=jnp.int32)
    used = position[None, :] < spoke_count[:, None]
    match = spoke_angle[:, None] == jnp.arange(angles, dtype=jnp.int32)[None, :]
    weights = (used[:, :, None] & match[None, :, :]).astype(BF16)
    binned = jnp.einsum("rpsn,psa->rpan", kdata[:, :, 0], weights, preferred_element_type=F32).astype(BF16)
    pieces = binned.reshape(2, parts, angles, segs, seg)
    contrib = jnp.einsum("rpagj,agjt->pragt", pieces, interp, preferred_element_type=F32).astype(BF16)
    hits = angles * segs
    contrib = contrib.reshape(parts, 2 * hits, seg)

    across = side // seg
    index = jnp.arange(side, dtype=jnp.int32)
    where = block_index.reshape(-1)
    hit_y = where // across
    hit_x = where % across
    cos_y, sin_y = cos_sin(index[:, None] * hit_y[None, :], side, F32)
    here = (jnp.arange(across, dtype=jnp.int32)[:, None, None] == hit_x).astype(F32)
    cos_y, sin_y = cos_y * here, sin_y * here
    ymat = jnp.concatenate(
        [jnp.concatenate([cos_y, sin_y], 2), jnp.concatenate([-sin_y, cos_y], 2)], 1
    ).astype(BF16)
    cos_x, sin_x = cos_sin(index[:, None] * index[None, :], side, F32)
    xmat = jnp.concatenate(
        [jnp.concatenate([cos_x, -sin_x], 1), jnp.concatenate([sin_x, cos_x], 1)], 0
    ).astype(BF16)
    low = jnp.arange(parts, dtype=jnp.int32)
    outward = jnp.where(kz < 2, 0, groups - 1)
    tables = []
    for owner in (kz, outward):
        tables += cos_sin(low[:, None] * (owner * parts + low)[None, :], length, F32)
    twiddle = jnp.stack(tables)

    assert groups == 4 and parts % groups == 0
    chunks = (rows // SUBLANE) * (side // LANE)
    block = (parts, 2, SUBLANE, LANE)
    vmem = pl.BlockSpec(memory_space=pltpu.VMEM)
    scratch = [
        pltpu.VMEM((chunks, coils) + block, F32),
        pltpu.VMEM((chunks, groups) + block, F32),
        pltpu.VMEM((chunks,) + block, F32),
        pltpu.VMEM((chunks,) + block, F32),
    ]
    scratch += [pltpu.VMEM((chunks, coils >> (s + 1)) + block, F32) for s in range(bits)]
    scratch += [pltpu.SemaphoreType.DMA((parts // SUB,))] * 2
    scratch += [pltpu.SemaphoreType.DMA((bits - 1, chunks))] * 2
    scratch += [pltpu.SemaphoreType.DMA((4, chunks))] * 2
    return pl.pallas_call(
        functools.partial(kernel, bits, groups, parts, rows, side),
        out_shape=jax.ShapeDtypeStruct((2, parts, rows, side), F32),
        in_specs=[vmem] * 4 + [pl.BlockSpec(memory_space=pltpu.SMEM)],
        out_specs=vmem,
        scratch_shapes=scratch,
        compiler_params=pltpu.CompilerParams(
            collective_id=0, has_side_effects=True, vmem_limit_bytes=60 * 1024 * 1024
        ),
        name="combine",
    )(contrib, ymat, xmat, sens_maps[:, 0], twiddle)


def solution(mesh):
    placed = (
        P(None, "kz", "coil", None, None),
        P(),
        P("kz"),
        P(),
        P(),
        P(None, "coil", None, None),
    )
    return jax.shard_map(
        per_device,
        mesh=mesh,
        in_specs=placed,
        out_specs=P(None, "kz", "coil", None),
        check_vma=False,
    )
```
